32 devices in a mesh: rep: 1, r: 4 (over z), s: 8 (over x, y, core).
Axes of the slice: x: 2, y: 2, z: 4, core: 2. Of those that a mesh axis runs over, the one named last changes fastest.
Arguments:
- x: bfloat16 [32, 4096, 768], P(('rep', 'r', 's'))
- dy: bfloat16 [32, 4096, 768], P(('rep', 'r', 's'))
- w_gate: bfloat16 [2, 768, 2304], P(None, 's')
- w_up: bfloat16 [2, 768, 2304], P(None, 's')
- w_down: bfloat16 [2, 2304, 768], P(None, 's')
Outputs:
- output 1: bfloat16 [32, 4096, 768], P(('rep', 'r', 's'))
- output 2: bfloat16 [2, 768, 2304], P('rep', 's')
- output 3: bfloat16 [2, 768, 2304], P('rep', 's')
- output 4: bfloat16 [2, 2304, 768], P('rep', 's')
All inputs are finite; a program needn't handle non-finite values.
Results may differ from the reference program's by a relative error of at most 0.018.
Values are sent between devices in bfloat16 or wider.
A program may use at most 2 GiB of HBM per device.

```python
import jax
import jax.numpy as jnp
from jax import lax

SEQUENCES = 32
TOKENS = 4096
D = 768
FF = 2304
LAYERS = 2
NAMES = ("w_gate", "w_up", "w_down")
SHAPES = {"w_gate": (LAYERS, D, FF), "w_up": (LAYERS, D, FF), "w_down": (LAYERS, FF, D)}


def bump(key, n, height):
    away = (jnp.arange(n, dtype=jnp.int32) - jax.random.randint(key, (), 0, n, jnp.int32)) % n
    return jnp.where(away < n // 8, height, 1.0)


def together(key, own, strength):
    shared = jax.random.normal(key, own.shape[1:], jnp.float32)
    return (own + strength * shared) * lax.rsqrt(1 + strength * strength)


def setup_inputs(seed: int = 0, part: int = 0) -> dict:
    kx, kdy, ka, kb, kz, kf, kh, kl, *kw = jax.random.split(jax.random.key(seed), 8 + len(NAMES))
    kx, kdy, ka, kb = (jax.random.fold_in(k, part) for k in (kx, kdy, ka, kb))
    shape = (SEQUENCES, TOKENS, D)
    much_x, much_dy = jax.random.uniform(kz, (2,), jnp.float32, 0.0, 1.0)
    layers = 2.0 ** jax.random.uniform(kl, (LAYERS, 1, 1), jnp.float32, -1.0, 1.0)
    x = together(ka, jax.random.normal(kx, shape, jnp.float32), much_x) * bump(kf, D, 4.0)
    dy = together(kb, jax.random.normal(kdy, shape, jnp.float32), much_dy)
    drawn = {"x": x.astype(jnp.bfloat16), "dy": (dy * (SEQUENCES * TOKENS) ** -0.5).astype(jnp.bfloat16)}
    for key, name in zip(kw, NAMES, strict=True):
        w = jax.random.normal(key, SHAPES[name], jnp.float32) * SHAPES[name][1] ** -0.5
        drawn[name] = (w * {"w_gate": 1.0, "w_up": bump(kh, FF, 4.0), "w_down": layers}[name]).astype(jnp.bfloat16)
    return drawn


def matmul(a, w):
    return jnp.dot(a, w, preferred_element_type=jnp.float32).astype(jnp.bfloat16)


def normed(h):
    wide = h.astype(jnp.float32)
    scale = lax.rsqrt(jnp.mean(wide**2, -1, keepdims=True) + 1e-6)
    return (wide * scale).astype(jnp.bfloat16)


def layer(h, w):
    a = normed(h)
    gate = jnp.dot(a, w["w_gate"], preferred_element_type=jnp.float32)
    up = jnp.dot(a, w["w_up"], preferred_element_type=jnp.float32)
    return h + matmul((jax.nn.silu(gate) * up).astype(jnp.bfloat16), w["w_down"])


def stack(weights, h):
    return lax.scan(lambda h, w: (layer(h, w), None), h, weights)[0]


def reference(x, dy, w_gate, w_up, w_down):
    weights = dict(zip(NAMES, (w_gate, w_up, w_down), strict=True))

    def take(so_far, sequence):
        h, by_y = sequence
        _, back = jax.vjp(stack, weights, h)
        by_weights, by_h = back(by_y)
        return jax.tree.map(lambda total, term: total + term.astype(jnp.float32), so_far, by_weights), by_h

    none_yet = {name: jnp.zeros(w.shape, jnp.float32) for name, w in weights.items()}
    by_weights, by_x = lax.scan(take, none_yet, (x, dy))
    return (by_x, *(by_weights[name].astype(jnp.bfloat16) for name in NAMES))
```

```python
import functools

import jax
import jax.numpy as jnp
from jax import lax
from jax.experimental import pallas as pl
from jax.experimental.pallas import tpu as pltpu
from jax.sharding import Mesh
from jax.sharding import PartitionSpec as P

BF, F32 = jnp.bfloat16, jnp.float32
TB = 1024
CB = 768
NN, NT, TN = ((1,), (0,)), ((1,), (1,)), ((0,), (0,))


def dot(a, b, dims=NN):
    return lax.dot_general(a, b, (dims, ((), ())), preferred_element_type=F32)


def normed(h):
    wide = h.astype(F32)
    return (wide * lax.rsqrt(jnp.mean(wide**2, -1, keepdims=True) + 1e-6)).astype(BF)


def call(kernel, grid, ins, outs, scratch=(), flops=0, aliases=None, name=None):
    def spec(block, index):
        return pl.BlockSpec(memory_space=pl.ANY) if block is None else pl.BlockSpec(block, index)

    size = sum(a.size * a.dtype.itemsize for a, *_ in ins)
    return pl.pallas_call(
        kernel,
        grid=grid,
        in_specs=[spec(b, i) for _, b, i in ins],
        out_specs=[spec(b, i) for *_, b, i in outs],
        out_shape=[jax.ShapeDtypeStruct(s, d) for s, d, *_ in outs],
        scratch_shapes=list(scratch),
        input_output_aliases=aliases or {},
        cost_estimate=pl.CostEstimate(flops=flops, bytes_accessed=size, transcendentals=0),
        compiler_params=pltpu.CompilerParams(vmem_limit_bytes=62 * 2**20, dimension_semantics=("arbitrary",) * len(grid)),
        name=name,
    )(*[a for a, *_ in ins])


def put_rows(w_ref, out, lanes=slice(None)):
    cores, chips, rows = w_ref.shape[:3]
    for chip in range(chips):
        for core in range(cores):
            out[pl.ds((chip * cores + core) * rows, rows), :] = w_ref[core, chip][:, lanes]


def norm_kernel(x_ref, a_ref):
    a_ref[...] = normed(x_ref[...])


def fwd_kernel(a_ref, wg_ref, wu_ref, gate_ref, up_ref, p_ref, wg, wu):
    @pl.when(pl.program_id(1) == 0)
    def _():
        put_rows(wg_ref, wg)
        put_rows(wu_ref, wu)

    a = a_ref[...]
    gate, up = dot(a, wg[...]), dot(a, wu[...])
    gate_ref[...], up_ref[...] = gate, up
    p_ref[...] = (gate * jax.nn.sigmoid(gate) * up).astype(BF)


def down_kernel(p_ref, x_ref, wd_ref, h_ref, a_ref, wd):
    @pl.when(pl.program_id(0) == 0)
    def _():
        put_rows(wd_ref, wd)

    h = x_ref[...] + dot(p_ref[...], wd[...]).astype(BF)
    h_ref[...] = h
    a_ref[...] = normed(h)


def gates(gate, up, dp):
    sig = jax.nn.sigmoid(gate)
    silu = gate * sig
    return silu, (dp * up * (sig + silu * (1 - sig))).astype(BF), (dp * silu).astype(BF)


def finish(dw_ref, acc, lanes=slice(None)):
    cores, chips, rows = dw_ref.shape[:3]
    for chip in range(chips):
        for core in range(cores):
            dw_ref[core, chip, :, lanes] = acc[pl.ds((chip * cores + core) * rows, rows), :].astype(BF)


def back_kernel(saved, chunk, *refs):
    refs = list(refs)
    a_ref, dh_ref, wd_ref = refs[:3]
    if saved:
        gate_ref, up_ref = refs[3:5]
    else:
        wg_ref, wu_ref = refs[3:5]
    refs = refs[5 + (chunk > 0) * (2 if saved else 3) :]
    dgate_ref, dup_ref, dw_ref = refs[:3]
    p_ref = None if saved else refs[3]
    accg, accu, wd, *rest = refs[3 if saved else 4 :]
    t = pl.program_id(0)

    @pl.when(t == 0)
    def _():
        accg[...] = jnp.zeros_like(accg)
        accu[...] = jnp.zeros_like(accu)
        put_rows(wd_ref, wd)
        if not saved:
            put_rows(wg_ref, rest[0])
            put_rows(wu_ref, rest[1])

    a, dh = a_ref[...], dh_ref[...]
    if saved:
        gate, up = gate_ref[...], up_ref[...]
    else:
        gate, up = dot(a, rest[0][...]), dot(a, rest[1][...])
    dp = dot(dh, wd[chunk * CB : (chunk + 1) * CB, :], NT).astype(BF).astype(F32)
    silu, dgate, dup = gates(gate, up, dp)
    dgate_ref[...], dup_ref[...] = dgate, dup
    if not saved:
        p_ref[...] = (silu * up).astype(BF)
    accg[...] += dot(a, dgate, TN)
    accu[...] += dot(a, dup, TN)

    @pl.when(t == pl.num_programs(0) - 1)
    def _():
        finish(dw_ref, accg, slice(0, CB))
        finish(dw_ref, accu, slice(CB, 2 * CB))


def down_back_kernel(p_ref, dh_ref, dw_ref, acc):
    t = pl.program_id(0)

    @pl.when(t == 0)
    def _():
        acc[...] = jnp.zeros_like(acc)

    acc[...] += dot(p_ref[...], dh_ref[...], TN)

    @pl.when(t == pl.num_programs(0) - 1)
    def _():
        finish(dw_ref, acc)


def input_back_kernel(dgate_ref, dup_ref, h_ref, dh_ref, wg_ref, wu_ref, out_ref, wg, wu):
    @pl.when(pl.program_id(0) == 0)
    def _():
        put_rows(wg_ref, wg)
        put_rows(wu_ref, wu)

    da = dot(dgate_ref[...], wg[...], NT).astype(BF) + dot(dup_ref[...], wu[...], NT).astype(BF)
    g, h = da.astype(F32), h_ref[...].astype(F32)
    scale = lax.rsqrt(jnp.mean(h**2, -1, keepdims=True) + 1e-6)
    dn = g * scale - h * (scale**3 * jnp.mean(g * h, -1, keepdims=True))
    out_ref[...] = dh_ref[...] + dn.astype(BF)


def solution(mesh):
    sizes = mesh.shape
    rep, r, s = sizes["rep"], sizes["r"], sizes["s"]
    chips, cores = s // 2, 2
    fine = Mesh(mesh.devices.reshape(rep, r, chips, cores), ("rep", "r", "chip", "core"))

    def gathered(w):
        return lax.all_gather(lax.all_gather(w, "chip"), "core")

    def scattered(term):
        return lax.psum_scatter(lax.psum_scatter(term, "core"), "chip")

    def step(x, dy, w_gate, w_up, w_down):
        x, dy = x[0], dy[0]
        tokens, d = x.shape
        layers, _, ff = w_gate.shape
        nt, nc = tokens // TB, ff // CB
        row, whole = (lambda t: (t, 0)), (lambda *_: (0, 0, 0, 0))
        rows_d, rows_f = d // s, ff // s
        mm = 2 * tokens * d * ff
        blockrow = (TB, d)
        gu = [gathered(jnp.concatenate([w_gate[l], w_up[l]], 1)) for l in range(layers)]
        wd = [gathered(w_down[l]) for l in range(layers)]
        wd_block = (cores, chips, rows_f, d)
        w_block = (cores, chips, rows_d, CB)
        w_half = (cores, chips, rows_d, ff)

        (a1,) = call(norm_kernel, (nt,), [(x, blockrow, row)], [((tokens, d), BF, blockrow, row)], flops=10**6, name="norm")
        gate, up, p1 = call(
            fwd_kernel,
            (nc, nt),
            [
                (a1, blockrow, lambda c, t: (t, 0)),
                (gu[0], w_block, lambda c, t: (0, 0, 0, c)),
                (gu[0], w_block, lambda c, t: (0, 0, 0, nc + c)),
            ],
            [((tokens, ff), dt, (TB, CB), lambda c, t: (t, c)) for dt in (F32, F32, BF)],
            [pltpu.VMEM((d, CB), BF)] * 2,
            2 * mm,
            name="fwd",
        )
        h1, a2 = call(
            down_kernel,
            (nt,),
            [(p1, (TB, ff), row), (x, blockrow, row), (wd[0], wd_block, whole)],
            [((tokens, d), BF, blockrow, row)] * 2,
            [pltpu.VMEM((ff, d), BF)],
            mm,
            name="down",
        )

        def back(l, a, dh, h, saved):
            scratch = [pltpu.VMEM((d, CB), F32)] * 2 + [pltpu.VMEM((ff, d), BF)]
            so_far, dgu = [], []
            for c in range(nc):
                ins = [(a, blockrow, row), (dh, blockrow, row), (wd[l], wd_block, whole)]
                here = lambda t, c=c: (t, c)
                if saved:
                    ins += [(gate, (TB, CB), here), (up, (TB, CB), here)]
                else:
                    ins += [(gu[l], w_block, lambda t, c=c: (0, 0, 0, c)), (gu[l], w_block, lambda t, c=c: (0, 0, 0, nc + c))]
                outs = [((tokens, ff), BF, (TB, CB), here)] * 2 + [((cores, chips, rows_d, 2 * CB), BF, (cores, chips, rows_d, 2 * CB), whole)]
                if not saved:
                    outs += [outs[0]]
                aliases = {}
                if c:
                    for i, buffer in enumerate(so_far):
                        aliases[len(ins)] = i if i < 2 else 3
                        ins.append((buffer, None, None))
                got = call(
                    functools.partial(back_kernel, saved, c),
                    (nt,),
                    ins,
                    outs,
                    scratch + ([] if saved else [pltpu.VMEM((d, CB), BF)] * 2),
                    (3 if saved else 5) * mm // nc,
                    aliases,
                    f"back{l}_{c}",
                )
                so_far = got[:2] + got[3:]
                dgu.append(got[2])
            dgate, dup = so_far[:2]
            p = p1 if saved else so_far[2]
            return dgate, dup, p, dgu

        def down_back(p, dh):
            return call(
                down_back_kernel,
                (nt,),
                [(p, (TB, ff), row), (dh, blockrow, row)],
                [((cores, chips, rows_f, d), BF, (cores, chips, rows_f, d), whole)],
                [pltpu.VMEM((ff, d), F32)],
                mm,
                name="down_back",
            )[0]

        def input_back(l, dgate, dup, h, dh):
            return call(
                input_back_kernel,
                (nt,),
                [
                    (dgate, (TB, ff), row),
                    (dup, (TB, ff), row),
                    (h, blockrow, row),
                    (dh, blockrow, row),
                    (gu[l], w_half, lambda t: (0, 0, 0, 0)),
                    (gu[l], w_half, lambda t: (0, 0, 0, 1)),
                ],
                [((tokens, d), BF, blockrow, row)],
                [pltpu.VMEM((d, ff), BF)] * 2,
                2 * mm,
                name="input_back",
            )[0]

        dgate, dup, p2, dgu2 = back(1, a2, dy, h1, False)
        dwd2 = down_back(p2, dy)
        dh1 = input_back(1, dgate, dup, h1, dy)
        mine2 = [scattered(t) for t in dgu2] + [scattered(dwd2)]
        mine2 = [lax.psum(t, "r") for t in mine2]
        dwd1 = down_back(p1, dh1)
        dgate, dup, _, dgu1 = back(0, a1, dh1, x, True)
        mine1 = [scattered(dwd1)] + [scattered(t) for t in dgu1]
        mine2, mine1 = lax.optimization_barrier((mine2, mine1))
        mine1 = [lax.psum(t, "r") for t in mine1]
        dx = input_back(0, dgate, dup, x, dh1)

        g = jnp.stack([jnp.concatenate([t[:, :CB] for t in m], 1) for m in (mine1[1:], mine2[:nc])])
        u = jnp.stack([jnp.concatenate([t[:, CB:] for t in m], 1) for m in (mine1[1:], mine2[:nc])])
        return dx[None], g, u, jnp.stack([mine1[0], mine2[nc]])

    states, cut = P(("rep", "r", "chip", "core"), None, None), P(None, ("chip", "core"), None)
    return jax.shard_map(
        step,
        mesh=fine,
        in_specs=(states, states) + (cut,) * 3,
        out_specs=(states,) + (P("rep", ("chip", "core"), None),) * 3,
        check_vma=False,
    )
```

```python
import functools

import jax
import jax.numpy as jnp
from jax import lax
from jax.experimental import pallas as pl
from jax.experimental.pallas import tpu as pltpu
from jax.sharding import Mesh
from jax.sharding import PartitionSpec as P

BF, F32 = jnp.bfloat16, jnp.float32
TB = 512
CB = 768
NN, NT, TN = ((1,), (0,)), ((1,), (1,)), ((0,), (0,))
MESH = pl.DeviceIdType.MESH
DMA = pltpu.SemaphoreType.DMA


def dot(a, b, dims=NN):
    return lax.dot_general(a, b, (dims, ((), ())), preferred_element_type=F32)


def normed(h):
    wide = h.astype(F32)
    return (wide * lax.rsqrt(jnp.mean(wide**2, -1, keepdims=True) + 1e-6)).astype(BF)


def chip_peers():
    chip = lax.axis_index("chip")
    return chip + 1 - 2 * lax.rem(chip, 2), lax.rem(chip + 2, 4), 3 - chip


def to_chip(peer, **kw):
    return pltpu.make_async_remote_copy(device_id={"chip": peer}, device_id_type=MESH, **kw)


def to_partner(**kw):
    return pltpu.make_async_remote_copy(device_id={"core": 1 - lax.axis_index("core")}, device_id_type=MESH, **kw)


def enter():
    barrier = pltpu.get_barrier_semaphore()
    for peer in chip_peers():
        pl.semaphore_signal(barrier, inc=1, device_id={"chip": peer}, device_id_type=MESH)
    pl.semaphore_signal(barrier, inc=1, device_id={"core": 1 - lax.axis_index("core")}, device_id_type=MESH)
    pl.semaphore_wait(barrier, 4)


class Gather:
    def __init__(self, *parts):
        self.rows, self.parts = parts[0][0].shape[1], parts
        self.ins = [(w, (1, *w.shape[1:]), lambda *_, l=l: (l, 0, 0)) for w, l, *_ in parts]
        self.outs = [((8 * self.rows, sum(p[3] for p in parts)), BF, None, None)]
        n = len(parts)
        self.scratch = [DMA((3, n)), DMA((3, n)), DMA((4, n)), DMA((4, n)), DMA((n,))]

    def bind(self, ins, outs, scratch):
        (self.full,) = outs
        chip, core = lax.axis_index("chip"), lax.axis_index("core")
        send, recv, psend, precv, local = scratch
        self.out, self.on, self.own, at = [], [], [], 0
        for k, (shard, (_, _, column, width)) in enumerate(zip(ins, self.parts)):

            def place(chip, core, at=at, width=width):
                first = pl.multiple_of((chip * 2 + core) * self.rows, self.rows)
                return self.full.at[pl.ds(first, self.rows), pl.ds(at, width)]

            mine, here = shard.at[0, :, pl.ds(column, width)], place(chip, core)
            self.own.append(to_partner(src_ref=mine, dst_ref=here, send_sem=psend.at[3, k], recv_sem=precv.at[3, k]))
            self.own.append(pltpu.make_async_copy(mine, here, local.at[k]))
            for i, peer in enumerate(chip_peers()):
                there = place(peer, core)
                self.out.append(to_chip(peer, src_ref=mine, dst_ref=here, send_sem=send.at[i, k], recv_sem=recv.at[i, k]))
                self.on.append(to_partner(src_ref=there, dst_ref=there, send_sem=psend.at[i, k], recv_sem=precv.at[i, k]))
            at += width

    def start(self):
        for copy in self.out + self.own:
            copy.start()

    def end(self):
        for copy, on in zip(self.out, self.on):
            copy.wait_recv()
            on.start()
        for copy in self.out:
            copy.wait_send()
        for copy in self.on + self.own:
            copy.wait()


class Scatter:
    def __init__(self, sums):
        self.ins = [(sums, None, None)]
        self.outs = [((3, *sums.shape[1:]), BF, None, None)]
        self.scratch = [DMA((3,)), DMA((3,))]

    def bind(self, ins, outs, scratch):
        self.out = [
            to_chip(peer, src_ref=ins[0].at[peer], dst_ref=outs[0].at[i], send_sem=scratch[0].at[i], recv_sem=scratch[1].at[i])
            for i, peer in enumerate(chip_peers())
        ]

    def start(self):
        for copy in self.out:
            copy.start()

    def end(self):
        for copy in self.out:
            copy.wait()


def pair_sum(acc, sums_ref, sent, got, send, recv):
    core = lax.axis_index("core")
    chips, rows = sums_ref.shape[:2]

    def rows_of(chip, core):
        return acc[pl.ds(pl.multiple_of((chip * 2 + core) * rows, rows), rows), :]

    for chip in range(chips):
        sent[chip] = rows_of(chip, 1 - core).astype(BF)
    copy = to_partner(src_ref=sent, dst_ref=got, send_sem=send, recv_sem=recv)
    copy.start()
    copy.wait()
    for chip in range(chips):
        sums_ref[chip] = (rows_of(chip, core) + got[chip].astype(F32)).astype(BF)


def pair_scratch(rows, n):
    return [pltpu.VMEM((4, rows, n), BF)] * 2 + [DMA, DMA]


def call(kernel, grid, ins, outs, scratch, flops, number, moves=(), aliases=None, steered=False, name=None):
    def spec(block, index):
        return pl.BlockSpec(memory_space=pl.ANY) if block is None else pl.BlockSpec(block, index)

    n_in, n_out, n_scratch = len(ins), len(outs), len(scratch)
    all_ins = list(ins) + [a for m in moves for a in m.ins]
    all_outs = list(outs) + [a for m in moves for a in m.outs]
    all_scratch = list(scratch) + [a for m in moves for a in m.scratch]

    def body(*refs):
        ins_, outs_, scratch_ = refs[: len(all_ins)], refs[len(all_ins) : len(all_ins) + len(all_outs)], refs[len(all_ins) + len(all_outs) :]
        i, o, c = n_in, n_out, n_scratch
        for m in moves:
            m.bind(ins_[i : i + len(m.ins)], outs_[o : o + len(m.outs)], scratch_[c : c + len(m.scratch)])
            i, o, c = i + len(m.ins), o + len(m.outs), c + len(m.scratch)
        first = functools.reduce(lambda a, b: a & b, [pl.program_id(k) == 0 for k in range(len(grid))])
        last = functools.reduce(lambda a, b: a & b, [pl.program_id(k) == grid[k] - 1 for k in range(len(grid))])

        if number is not None:

            @pl.when(first)
            def _():
                enter()
                for m in moves:
                    m.start()

        kernel(*ins_[:n_in], *outs_[:n_out], *scratch_[:n_scratch], *(moves if steered else ()))

        if not steered:

            @pl.when(last)
            def _():
                for m in moves:
                    m.end()

    size = sum(a.size * a.dtype.itemsize for a, *_ in ins)
    return pl.pallas_call(
        body,
        grid=grid,
        in_specs=[spec(b, i) for _, b, i in all_ins],
        out_specs=[spec(b, i) for *_, b, i in all_outs],
        out_shape=[jax.ShapeDtypeStruct(s, d) for s, d, *_ in all_outs],
        scratch_shapes=all_scratch,
        input_output_aliases=aliases or {},
        cost_estimate=pl.CostEstimate(flops=flops, bytes_accessed=size, transcendentals=0),
        compiler_params=pltpu.CompilerParams(
            vmem_limit_bytes=62 * 2**20,
            dimension_semantics=("arbitrary",) * len(grid),
            collective_id=number,
            has_side_effects=number is not None,
        ),
        name=name,
    )(*[a for a, *_ in all_ins])


def fwd_kernel(x_ref, gate_ref, up_ref, p_ref, a_ref, w, a_all, local, *moves):
    c, t = pl.program_id(0), pl.program_id(1)
    *chunks, down = moves
    for i, chunk in enumerate(chunks):

        @pl.when((c == i) & (t == 0))
        def _():
            chunk.end()
            copy = pltpu.make_async_copy(chunk.full, w, local)
            copy.start()
            copy.wait()

    rows = pl.ds(pl.multiple_of(t * TB, TB), TB)

    @pl.when(c == 0)
    def _():
        a = normed(x_ref[...])
        a_ref[...] = a
        a_all[rows, :] = a

    a = a_all[rows, :]
    gate, up = dot(a, w[:, :CB]), dot(a, w[:, CB:])
    gate_ref[...], up_ref[...] = gate, up
    p_ref[...] = (gate * jax.nn.sigmoid(gate) * up).astype(BF)

    @pl.when((c == len(chunks) - 1) & (t == pl.num_programs(1) - 1))
    def _():
        down.end()


def down_kernel(p_ref, x_ref, wd_ref, h_ref, a_ref):
    h = x_ref[...] + dot(p_ref[...], wd_ref[...]).astype(BF)
    h_ref[...] = h
    a_ref[...] = normed(h)


def back_kernel(saved, n_alias, *refs):
    refs = list(refs)
    a_ref, dh_ref, wd_ref = refs[:3]
    given = refs[3:5] if saved else refs[3:4]
    refs = refs[3 + len(given) + n_alias :]
    d_ref = refs.pop(0)
    p_ref = None if saved else refs.pop(0)
    sums_ref, acc, *pair = refs
    t = pl.program_id(0)

    @pl.when(t == 0)
    def _():
        acc[...] = jnp.zeros_like(acc)

    a, dh = a_ref[...], dh_ref[...]
    if saved:
        gate, up = given[0][...], given[1][...]
    else:
        gate, up = dot(a, given[0][:, :CB]), dot(a, given[0][:, CB:])
    dp = dot(dh, wd_ref[...], NT).astype(BF).astype(F32)
    sig = jax.nn.sigmoid(gate)
    silu = gate * sig
    d_ref[:, :CB] = (dp * up * (sig + silu * (1 - sig))).astype(BF)
    d_ref[:, CB:] = (dp * silu).astype(BF)
    if not saved:
        p_ref[...] = (silu * up).astype(BF)
    acc[...] += dot(a, d_ref[...], TN)

    @pl.when(t == pl.num_programs(0) - 1)
    def _():
        pair_sum(acc, sums_ref, *pair)


def down_back_kernel(p_ref, dh_ref, sums_ref, acc, *pair):
    t = pl.program_id(0)

    @pl.when(t == 0)
    def _():
        acc[...] = jnp.zeros_like(acc)

    acc[...] += dot(p_ref[...], dh_ref[...], TN)

    @pl.when(t == pl.num_programs(0) - 1)
    def _():
        pair_sum(acc, sums_ref, *pair)


def input_back_kernel(d_ref, h_ref, dh_ref, *refs):
    *weights, out_ref = refs
    da = sum(dot(d_ref[:, 2 * CB * c : 2 * CB * (c + 1)], w[...], NT) for c, w in enumerate(weights)).astype(BF)
    g, h = da.astype(F32), h_ref[...].astype(F32)
    scale = lax.rsqrt(jnp.mean(h**2, -1, keepdims=True) + 1e-6)
    dn = g * scale - h * (scale**3 * jnp.mean(g * h, -1, keepdims=True))
    out_ref[...] = dh_ref[...] + dn.astype(BF)


def solution(mesh):
    sizes = mesh.shape
    rep, r, s = sizes["rep"], sizes["r"], sizes["s"]
    fine = Mesh(mesh.devices.reshape(rep, r, s // 2, 2), ("rep", "r", "chip", "core"))

    def step(x, dy, w_gate, w_up, w_down):
        x, dy = x[0], dy[0]
        tokens, d = x.shape
        layers, _, ff = w_gate.shape
        nt, nc = tokens // TB, ff // CB
        row = lambda t: (t, 0)
        rows_d, rows_f = d // s, ff // s
        mm = 2 * tokens * d * ff
        blockrow = (TB, d)
        state = ((tokens, d), BF, blockrow, row)
        numbers = iter(range(100))

        def chunk(l, c):
            return Gather((w_gate, l, c * CB, CB), (w_up, l, c * CB, CB))

        def down(l):
            return Gather((w_down, l, 0, d))

        last = lambda c, t: (jnp.where(c == 0, t, nt - 1), 0)
        gate, up, p1, a1, *full1 = call(
            fwd_kernel,
            (nc, nt),
            [(x, blockrow, last)],
            [((tokens, ff), dt, (TB, CB), lambda c, t: (t, c)) for dt in (F32, F32, BF)] + [((tokens, d), BF, blockrow, last)],
            [pltpu.VMEM((d, 2 * CB), BF), pltpu.VMEM((tokens, d), BF), DMA],
            2 * mm,
            next(numbers),
            [chunk(0, c) for c in range(nc)] + [down(0)],
            steered=True,
            name="fwd",
        )
        gu1, wd1 = full1[:nc], full1[nc]
        h1, a2, wd2, gu2_0 = call(
            down_kernel,
            (nt,),
            [(p1, (TB, ff), row), (x, blockrow, row), (wd1, (ff, d), lambda t: (0, 0))],
            [state] * 2,
            [],
            mm,
            next(numbers),
            [down(1), chunk(1, 0)],
            name="down",
        )

        def back(c, a, dh, wd, so_far, moves, w=None):
            here = lambda t: (t, c)
            ins = [(a, blockrow, row), (dh, blockrow, row), (wd, (CB, d), lambda t: (c, 0))]
            outs = [((tokens, 2 * ff), BF, (TB, 2 * CB), here)]
            if w is None:
                ins += [(gate, (TB, CB), here), (up, (TB, CB), here)]
            else:
                ins += [(w, (d, 2 * CB), lambda t: (0, 0))]
                outs += [((tokens, ff), BF, (TB, CB), here)]
            aliases = {len(ins) + i: i for i in range(len(so_far))}
            ins += [(buffer, None, None) for buffer in so_far]
            n = len(outs)
            outs += [((4, rows_d, 2 * CB), BF, (4, rows_d, 2 * CB), lambda t: (0, 0, 0))]
            got = call(
                functools.partial(back_kernel, w is None, len(so_far)),
                (nt,),
                ins,
                outs,
                [pltpu.VMEM((d, 2 * CB), F32)] + pair_scratch(rows_d, 2 * CB),
                (3 if w is None else 5) * mm // nc,
                next(numbers),
                moves,
                aliases,
                name="back",
            )
            return got[:n], got[n], got[n + 1 :]

        def down_back(p, dh, moves):
            return call(
                down_back_kernel,
                (nt,),
                [(p, (TB, ff), row), (dh, blockrow, row)],
                [((4, rows_f, d), BF, (4, rows_f, d), lambda t: (0, 0, 0))],
                [pltpu.VMEM((ff, d), F32)] + pair_scratch(rows_f, d),
                mm,
                next(numbers),
                moves,
                name="down_back",
            )

        def input_back(dgu, h, dh, ws, moves=()):
            return call(
                input_back_kernel,
                (nt,),
                [(dgu, (TB, 2 * ff), row), (h, blockrow, row), (dh, blockrow, row)] + [(w, w.shape, lambda t: (0, 0)) for w in ws],
                [state],
                [],
                2 * mm,
                next(numbers) if moves else None,
                moves,
                name="input_back",
            )

        def own(sums):
            return lax.dynamic_index_in_dim(sums, lax.axis_index("chip"), keepdims=False)

        def exchanged(sums):
            at = lax.axis_index("chip")
            perms = [[(i, i ^ m) for i in range(s // 2)] for m in (1, 2, 3)]
            return [lax.ppermute(lax.dynamic_index_in_dim(sums, at ^ m, keepdims=False), "chip", p) for m, p in zip((1, 2, 3), perms)]

        def mine(sums, arrived):
            return (own(sums).astype(F32) + jnp.sum(arrived.astype(F32), 0)).astype(BF)

        def total(terms, after):
            if after:
                after, terms = lax.optimization_barrier((after, terms))
            return [lax.psum(t, "r") for t in terms], after

        so_far, s20, (gu2_1, gu2_2) = back(0, a2, dy, wd2, [], [chunk(1, 1), chunk(1, 2)], gu2_0)
        so_far, s21, (r20,) = back(1, a2, dy, wd2, so_far, [Scatter(s20)], gu2_1)
        (dgu2, p2), s22, (r21,) = back(2, a2, dy, wd2, so_far, [Scatter(s21)], gu2_2)
        s2d, r22 = down_back(p2, dy, [Scatter(s22)])
        dh1, r2d = input_back(dgu2, h1, dy, [gu2_0, gu2_1, gu2_2], [Scatter(s2d)])
        terms = [mine(*wave) for wave in ((s20, r20), (s21, r21), (s22, r22), (s2d, r2d))]
        dh1, terms = lax.optimization_barrier((dh1, terms))
        t2, _ = total(terms, [])
        (s1d,) = down_back(p1, dh1, [])
        so_far, s10, (r1d,) = back(0, a1, dh1, wd1, [], [Scatter(s1d)])
        so_far, s11, (r10,) = back(1, a1, dh1, wd1, so_far, [Scatter(s10)])
        so_far, t2 = lax.optimization_barrier((so_far, t2))
        t1a, t2 = total([mine(s1d, r1d)], t2)
        (dgu1,), s12, (r11,) = back(2, a1, dh1, wd1, so_far, [Scatter(s11)])
        t1b, t1a = total([mine(s10, r10), mine(s11, r11)], t1a)
        others = exchanged(s12)
        dx = input_back(dgu1, x, dh1, gu1)[0]
        dx, others = lax.optimization_barrier((dx, others))
        (t1c,), t1b = total([(own(s12).astype(F32) + sum(t.astype(F32) for t in others)).astype(BF)], t1b)

        def halves(terms, i):
            return jnp.concatenate([t[:, i * CB : (i + 1) * CB] for t in terms], 1)

        dgu = [[*t1b, t1c], t2[:nc]]
        return dx[None], *(jnp.stack([halves(t, i) for t in dgu]) for i in range(2)), jnp.stack([t1a[0], t2[nc]])

    states, cut = P(("rep", "r", "chip", "core"), None, None), P(None, ("chip", "core"), None)
    return jax.shard_map(
        step,
        mesh=fine,
        in_specs=(states, states) + (cut,) * 3,
        out_specs=(states,) + (P("rep", ("chip", "core"), None),) * 3,
        check_vma=False,
    )
```

```python
import functools

import jax
import jax.numpy as jnp
from jax import lax
from jax.experimental import pallas as pl
from jax.experimental.pallas import tpu as pltpu
from jax.sharding import Mesh
from jax.sharding import PartitionSpec as P

BF, F32 = jnp.bfloat16, jnp.float32
TB = 512
CB = 768
NN, NT, TN = ((1,), (0,)), ((1,), (1,)), ((0,), (0,))
MESH = pl.DeviceIdType.MESH
DMA = pltpu.SemaphoreType.DMA


def dot(a, b, dims=NN):
    return lax.dot_general(a, b, (dims, ((), ())), preferred_element_type=F32)


def normed(h):
    wide = h.astype(F32)
    return (wide * lax.rsqrt(jnp.mean(wide**2, -1, keepdims=True) + 1e-6)).astype(BF)


def chip_peers():
    chip = lax.axis_index("chip")
    return chip + 1 - 2 * lax.rem(chip, 2), lax.rem(chip + 2, 4), 3 - chip


def z_peers():
    z = lax.axis_index("r")
    return z + 1 - 2 * lax.rem(z, 2), lax.rem(z + 2, 4)


def to_z(peer, **kw):
    return pltpu.make_async_remote_copy(device_id={"r": peer}, device_id_type=MESH, **kw)


def to_chip(peer, **kw):
    return pltpu.make_async_remote_copy(device_id={"chip": peer}, device_id_type=MESH, **kw)


def to_partner(**kw):
    return pltpu.make_async_remote_copy(device_id={"core": 1 - lax.axis_index("core")}, device_id_type=MESH, **kw)


def enter():
    barrier = pltpu.get_barrier_semaphore()
    for peer in chip_peers():
        pl.semaphore_signal(barrier, inc=1, device_id={"chip": peer}, device_id_type=MESH)
    pl.semaphore_signal(barrier, inc=1, device_id={"core": 1 - lax.axis_index("core")}, device_id_type=MESH)
    for peer in z_peers():
        pl.semaphore_signal(barrier, inc=1, device_id={"r": peer}, device_id_type=MESH)
    pl.semaphore_wait(barrier, 6)


class Gather:
    def __init__(self, *parts):
        self.rows, self.parts = parts[0][0].shape[1], parts
        self.ins = [(w, (1, *w.shape[1:]), lambda *_, l=l: (l, 0, 0)) for w, l, *_ in parts]
        self.outs = [((8 * self.rows, sum(p[3] for p in parts)), BF, None, None)]
        n = len(parts)
        self.scratch = [DMA((3, n)), DMA((3, n)), DMA((4, n)), DMA((4, n)), DMA((n,))]

    def bind(self, ins, outs, scratch):
        (self.full,) = outs
        chip, core = lax.axis_index("chip"), lax.axis_index("core")
        send, recv, psend, precv, local = scratch
        self.out, self.on, self.own, at = [], [], [], 0
        for k, (shard, (_, _, column, width)) in enumerate(zip(ins, self.parts)):

            def place(chip, core, at=at, width=width):
                first = pl.multiple_of((chip * 2 + core) * self.rows, self.rows)
                return self.full.at[pl.ds(first, self.rows), pl.ds(at, width)]

            mine, here = shard.at[0, :, pl.ds(column, width)], place(chip, core)
            self.own.append(to_partner(src_ref=mine, dst_ref=here, send_sem=psend.at[3, k], recv_sem=precv.at[3, k]))
            self.own.append(pltpu.make_async_copy(mine, here, local.at[k]))
            for i, peer in enumerate(chip_peers()):
                there = place(peer, core)
                self.out.append(to_chip(peer, src_ref=mine, dst_ref=here, send_sem=send.at[i, k], recv_sem=recv.at[i, k]))
                self.on.append(to_partner(src_ref=there, dst_ref=there, send_sem=psend.at[i, k], recv_sem=precv.at[i, k]))
            at += width

    def before(self, step, steps):
        if step == 0:
            for copy in self.out + self.own:
                copy.start()

    def after(self, step, steps):
        if step == steps - 1:
            self.forward()
            self.finish()

    def forward(self):
        for copy, on in zip(self.out, self.on):
            copy.wait_recv()
            on.start()

    def finish(self):
        for copy in self.out:
            copy.wait_send()
        for copy in self.on + self.own:
            copy.wait()


class Reduce:
    def __init__(self, source, *stages):
        self.stages, shape = stages, source.shape[-2:]
        self.ins = [(source, None, None)]
        self.outs = [(shape, BF, shape, lambda *_: (0, 0))]
        n = len(stages)
        self.scratch = [pltpu.VMEM((n, *shape), BF), DMA]
        for kind, _ in stages:
            k = 3 if kind == "chips" else 1
            self.scratch += [pltpu.VMEM((k, *shape), BF), DMA((k,)), DMA((k,))]

    def bind(self, ins, outs, scratch):
        (source,), (self.result,) = ins, outs
        self.own, local, *rest = scratch
        first = source.at[lax.axis_index("chip")] if self.stages[0][0] == "chips" else source
        self.load = pltpu.make_async_copy(first, self.own.at[0], local)
        self.copies, self.got = [], []
        for j, (kind, _) in enumerate(self.stages):
            got, send, recv = rest[3 * j : 3 * j + 3]
            self.got.append(got)
            if kind == "chips":
                self.copies.append(
                    [
                        to_chip(peer, src_ref=source.at[peer], dst_ref=got.at[i], send_sem=send.at[i], recv_sem=recv.at[i])
                        for i, peer in enumerate(chip_peers())
                    ]
                )
            else:
                here = source if j == 0 else self.own.at[j]
                self.copies.append([to_z(z_peers()[kind], src_ref=here, dst_ref=got.at[0], send_sem=send.at[0], recv_sem=recv.at[0])])

    def add(self, j):
        if j == 0:
            self.load.wait()
        for copy in self.copies[j]:
            copy.wait()
        total = self.own[j].astype(F32)
        for i in range(len(self.copies[j])):
            total += self.got[j][i].astype(F32)
        if j + 1 < len(self.stages):
            self.own[j + 1] = total.astype(BF)
        else:
            self.result[...] = total.astype(BF)

    def before(self, step, steps):
        if step == 0:
            self.load.start()
            for copy in self.copies[0]:
                copy.start()
        for j, (_, when) in enumerate(self.stages):
            if when == step:
                self.add(j)

    def after(self, step, steps):
        for j, (_, when) in enumerate(self.stages):
            if when == step:
                for copy in self.copies[j + 1]:
                    copy.start()
            if when is None and step == steps - 1:
                self.add(j)


def pair_sum(acc, sums_ref, sent, got, send, recv):
    core = lax.axis_index("core")
    chips, rows = sums_ref.shape[:2]

    def rows_of(chip, core):
        return acc[pl.ds(pl.multiple_of((chip * 2 + core) * rows, rows), rows), :]

    for chip in range(chips):
        sent[chip] = rows_of(chip, 1 - core).astype(BF)
    copy = to_partner(src_ref=sent, dst_ref=got, send_sem=send, recv_sem=recv)
    copy.start()
    copy.wait()
    for chip in range(chips):
        sums_ref[chip] = (rows_of(chip, core) + got[chip].astype(F32)).astype(BF)


def pair_scratch(rows, n):
    return [pltpu.VMEM((4, rows, n), BF)] * 2 + [DMA, DMA]


def call(kernel, grid, ins, outs, scratch, flops, number, moves=(), aliases=None, steered=False, name=None):
    def spec(block, index):
        return pl.BlockSpec(memory_space=pl.ANY) if block is None else pl.BlockSpec(block, index)

    n_in, n_out, n_scratch = len(ins), len(outs), len(scratch)
    all_ins = list(ins) + [a for m in moves for a in m.ins]
    all_outs = list(outs) + [a for m in moves for a in m.outs]
    all_scratch = list(scratch) + [a for m in moves for a in m.scratch]

    def body(*refs):
        ins_, outs_, scratch_ = refs[: len(all_ins)], refs[len(all_ins) : len(all_ins) + len(all_outs)], refs[len(all_ins) + len(all_outs) :]
        i, o, c = n_in, n_out, n_scratch
        for m in moves:
            m.bind(ins_[i : i + len(m.ins)], outs_[o : o + len(m.outs)], scratch_[c : c + len(m.scratch)])
            i, o, c = i + len(m.ins), o + len(m.outs), c + len(m.scratch)
        if number is not None:

            @pl.when(functools.reduce(lambda a, b: a & b, [pl.program_id(k) == 0 for k in range(len(grid))]))
            def _():
                enter()

        if steered or not moves:
            kernel(*ins_[:n_in], *outs_[:n_out], *scratch_[:n_scratch], *moves)
            return

        def at_steps(do):
            for step in steps:

                @pl.when(pl.program_id(0) == step)
                def _():
                    for m in moves:
                        getattr(m, do)(step, grid[0])

        steps = sorted({0, grid[0] - 1} | {when for m in moves for _, when in getattr(m, "stages", ()) if when is not None})
        at_steps("before")
        kernel(*ins_[:n_in], *outs_[:n_out], *scratch_[:n_scratch])
        at_steps("after")

    size = sum(a.size * a.dtype.itemsize for a, *_ in ins)
    return pl.pallas_call(
        body,
        grid=grid,
        in_specs=[spec(b, i) for _, b, i in all_ins],
        out_specs=[spec(b, i) for *_, b, i in all_outs],
        out_shape=[jax.ShapeDtypeStruct(s, d) for s, d, *_ in all_outs],
        scratch_shapes=all_scratch,
        input_output_aliases=aliases or {},
        cost_estimate=pl.CostEstimate(flops=flops, bytes_accessed=size, transcendentals=0),
        compiler_params=pltpu.CompilerParams(
            vmem_limit_bytes=62 * 2**20,
            dimension_semantics=("arbitrary",) * len(grid),
            collective_id=number,
            has_side_effects=number is not None,
        ),
        name=name,
    )(*[a for a, *_ in all_ins])


def fwd_kernel(x_ref, gate_ref, up_ref, p_ref, a_ref, h_ref, a2_ref, w, wd, a_all, p_all, local, *moves):
    c, t = pl.program_id(0), pl.program_id(1)
    nt, nc = pl.num_programs(1), len(moves) - 3
    late = 2

    def fetch(full, to):
        copy = pltpu.make_async_copy(full, to, local)
        copy.start()
        copy.wait()

    for i, move in enumerate(moves):

        @pl.when((c == 0) & (t == 0))
        def _():
            move.before(0, 1)
            if i == 0:
                move.forward()

        if 0 < i <= nc:

            @pl.when((c == i - 1) & (t == nt - late))
            def _():
                move.forward()

        if i <= nc:

            @pl.when((c == i) & (t == 0))
            def _():
                move.finish()
                fetch(move.full, w if i < nc else wd)

    rows = pl.ds(pl.multiple_of(t * TB, TB), TB)

    @pl.when(c == 0)
    def _():
        a = normed(x_ref[...])
        a_ref[...] = a
        a_all[rows, :] = a

    @pl.when(c < nc)
    def _():
        a = a_all[rows, :]
        gate, up = dot(a, w[:, :CB]), dot(a, w[:, CB:])
        gate_ref[...], up_ref[...] = gate, up
        p = (gate * jax.nn.sigmoid(gate) * up).astype(BF)
        p_ref[...] = p
        p_all[jnp.minimum(c, nc - 1), rows, :] = p

    @pl.when(c == nc)
    def _():
        h = x_ref[...] + sum(dot(p_all[i, rows, :], wd[i * CB : (i + 1) * CB, :]) for i in range(nc)).astype(BF)
        h_ref[...] = h
        a2_ref[...] = normed(h)

        @pl.when(t == nt - 1)
        def _():
            for move in moves[nc + 1 :]:
                move.forward()
            for move in moves[nc + 1 :]:
                move.finish()


def back_kernel(saved, n_alias, *refs):
    refs = list(refs)
    a_ref, dh_ref, wd_ref = refs[:3]
    given = refs[3:5] if saved else refs[3:4]
    refs = refs[3 + len(given) + n_alias :]
    d_ref = refs.pop(0)
    p_ref = None if saved else refs.pop(0)
    sums_ref, acc, *pair = refs
    t = pl.program_id(0)

    @pl.when(t == 0)
    def _():
        acc[...] = jnp.zeros_like(acc)

    a, dh = a_ref[...], dh_ref[...]
    if saved:
        gate, up = given[0][...], given[1][...]
    else:
        gate, up = dot(a, given[0][:, :CB]), dot(a, given[0][:, CB:])
    dp = dot(dh, wd_ref[...], NT).astype(BF).astype(F32)
    sig = jax.nn.sigmoid(gate)
    silu = gate * sig
    d_ref[:, :CB] = (dp * up * (sig + silu * (1 - sig))).astype(BF)
    d_ref[:, CB:] = (dp * silu).astype(BF)
    if not saved:
        p_ref[...] = (silu * up).astype(BF)
    acc[...] += dot(a, d_ref[...], TN)

    @pl.when(t == pl.num_programs(0) - 1)
    def _():
        pair_sum(acc, sums_ref, *pair)


def down_back_kernel(p_ref, dh_ref, sums_ref, acc, *pair):
    t = pl.program_id(0)

    @pl.when(t == 0)
    def _():
        acc[...] = jnp.zeros_like(acc)

    acc[...] += dot(p_ref[...], dh_ref[...], TN)

    @pl.when(t == pl.num_programs(0) - 1)
    def _():
        pair_sum(acc, sums_ref, *pair)


def input_back_kernel(d_ref, h_ref, dh_ref, *refs):
    *weights, out_ref = refs
    da = sum(dot(d_ref[:, 2 * CB * c : 2 * CB * (c + 1)], w[...], NT) for c, w in enumerate(weights)).astype(BF)
    g, h = da.astype(F32), h_ref[...].astype(F32)
    scale = lax.rsqrt(jnp.mean(h**2, -1, keepdims=True) + 1e-6)
    dn = g * scale - h * (scale**3 * jnp.mean(g * h, -1, keepdims=True))
    out_ref[...] = dh_ref[...] + dn.astype(BF)


def stack_kernel(*refs):
    *chunks, d0, d1, dg, du, dd = refs
    nc = len(chunks) // 2
    for i, ref in enumerate(chunks):
        at = slice(i % nc * CB, (i % nc + 1) * CB)
        dg[i // nc, :, at] = ref[:, :CB]
        du[i // nc, :, at] = ref[:, CB:]
    dd[0], dd[1] = d0[...], d1[...]


def solution(mesh):
    sizes = mesh.shape
    rep, r, s = sizes["rep"], sizes["r"], sizes["s"]
    fine = Mesh(mesh.devices.reshape(rep, r, s // 2, 2), ("rep", "r", "chip", "core"))

    def step(x, dy, w_gate, w_up, w_down):
        x, dy = x[0], dy[0]
        tokens, d = x.shape
        layers, _, ff = w_gate.shape
        nt, nc = tokens // TB, ff // CB
        row = lambda t: (t, 0)
        rows_d, rows_f = d // s, ff // s
        mm = 2 * tokens * d * ff
        blockrow = (TB, d)
        state = ((tokens, d), BF, blockrow, row)
        numbers = iter(range(100))

        def chunk(l, c):
            return Gather((w_gate, l, c * CB, CB), (w_up, l, c * CB, CB))

        def down(l):
            return Gather((w_down, l, 0, d))

        first = lambda c, t: (jnp.where(c == 0, t, nt - 1), 0)
        ends = lambda c, t: (jnp.where((c == 0) | (c == nc), t, nt - 1), 0)
        then = lambda c, t: (jnp.where(c == nc, t, 0), 0)
        chunked = lambda c, t: (jnp.where(c < nc, t, nt - 1), jnp.minimum(c, nc - 1))
        gate, up, p1, a1, h1, a2, *full = call(
            fwd_kernel,
            (nc + 1, nt),
            [(x, blockrow, ends)],
            [((tokens, ff), dt, (TB, CB), chunked) for dt in (F32, F32, BF)] + [((tokens, d), BF, blockrow, i) for i in (first, then, then)],
            [pltpu.VMEM((d, 2 * CB), BF), pltpu.VMEM((ff, d), BF), pltpu.VMEM((tokens, d), BF), pltpu.VMEM((nc, tokens, CB), BF), DMA],
            3 * mm,
            next(numbers),
            [chunk(0, c) for c in range(nc)] + [down(0), down(1), chunk(1, 0)],
            steered=True,
            name="fwd",
        )
        gu1, (wd1, wd2, gu2_0) = full[:nc], full[nc:]

        def back(c, a, dh, wd, so_far, moves, w=None):
            here = lambda t: (t, c)
            ins = [(a, blockrow, row), (dh, blockrow, row), (wd, (CB, d), lambda t: (c, 0))]
            outs = [((tokens, 2 * ff), BF, (TB, 2 * CB), here)]
            if w is None:
                ins += [(gate, (TB, CB), here), (up, (TB, CB), here)]
            else:
                ins += [(w, (d, 2 * CB), lambda t: (0, 0))]
                outs += [((tokens, ff), BF, (TB, CB), here)]
            aliases = {len(ins) + i: i for i in range(len(so_far))}
            ins += [(buffer, None, None) for buffer in so_far]
            n = len(outs)
            outs += [((4, rows_d, 2 * CB), BF, (4, rows_d, 2 * CB), lambda t: (0, 0, 0))]
            got = call(
                functools.partial(back_kernel, w is None, len(so_far)),
                (nt,),
                ins,
                outs,
                [pltpu.VMEM((d, 2 * CB), F32)] + pair_scratch(rows_d, 2 * CB),
                (3 if w is None else 5) * mm // nc,
                next(numbers),
                moves,
                aliases,
                name="back",
            )
            return got[:n], got[n], got[n + 1 :]

        def down_back(p, dh, moves):
            return call(
                down_back_kernel,
                (nt,),
                [(p, (TB, ff), row), (dh, blockrow, row)],
                [((4, rows_f, d), BF, (4, rows_f, d), lambda t: (0, 0, 0))],
                [pltpu.VMEM((ff, d), F32)] + pair_scratch(rows_f, d),
                mm,
                next(numbers),
                moves,
                name="down_back",
            )

        def input_back(dgu, h, dh, ws, moves=()):
            return call(
                input_back_kernel,
                (nt,),
                [(dgu, (TB, 2 * ff), row), (h, blockrow, row), (dh, blockrow, row)] + [(w, w.shape, lambda t: (0, 0)) for w in ws],
                [state],
                [],
                2 * mm,
                next(numbers) if moves else None,
                moves,
                name="input_back",
            )

        so_far, s20, (gu2_1, gu2_2) = back(0, a2, dy, wd2, [], [chunk(1, 1), chunk(1, 2)], gu2_0)
        so_far, s21, (u20,) = back(1, a2, dy, wd2, so_far, [Reduce(s20, ("chips", None))], gu2_1)
        (dgu2, p2), s22, (t20, u21) = back(
            2, a2, dy, wd2, so_far, [Reduce(u20, (0, 3), (1, None)), Reduce(s21, ("chips", None))], gu2_2
        )
        s2d, t21, u22 = down_back(p2, dy, [Reduce(u21, (0, 3), (1, None)), Reduce(s22, ("chips", None))])
        dh1, t22, u2d = input_back(dgu2, h1, dy, [gu2_0, gu2_1, gu2_2], [Reduce(u22, (0, 3), (1, None)), Reduce(s2d, ("chips", None))])
        s1d, v2d = down_back(p1, dh1, [Reduce(u2d, (0, None))])
        so_far, s10, (t2d, u1d) = back(0, a1, dh1, wd1, [], [Reduce(v2d, (1, None)), Reduce(s1d, ("chips", None))])
        so_far, s11, (v1d, u10) = back(1, a1, dh1, wd1, so_far, [Reduce(u1d, (0, None)), Reduce(s10, ("chips", None))])
        (dgu1,), s12, (t1d, v10, u11) = back(
            2, a1, dh1, wd1, so_far, [Reduce(v1d, (1, None)), Reduce(u10, (0, None)), Reduce(s11, ("chips", None))]
        )
        dx, t10, t11, t12 = input_back(
            dgu1, x, dh1, gu1, [Reduce(v10, (1, None)), Reduce(u11, (0, 2), (1, None)), Reduce(s12, ("chips", 3), (0, 5), (1, None))]
        )

        w_out = [((layers, rows_d, ff), BF)] * 2 + [((layers, rows_f, d), BF)]
        terms = (t10, t11, t12, t20, t21, t22, t1d, t2d)
        dg, du, dd = call(
            stack_kernel,
            (1,),
            [(t, t.shape, lambda _: (0, 0)) for t in terms],
            [(shape, dt, shape, lambda _: (0, 0, 0)) for shape, dt in w_out],
            [],
            10**6,
            None,
            name="stack",
        )
        return dx[None], dg, du, dd

    states, cut = P(("rep", "r", "chip", "core"), None, None), P(None, ("chip", "core"), None)
    return jax.shard_map(
        step,
        mesh=fine,
        in_specs=(states, states) + (cut,) * 3,
        out_specs=(states,) + (P("rep", ("chip", "core"), None),) * 3,
        check_vma=False,
    )
```

```python
import functools

import jax
import jax.numpy as jnp
from jax import lax
from jax.experimental import pallas as pl
from jax.experimental.pallas import tpu as pltpu
from jax.sharding import Mesh
from jax.sharding import PartitionSpec as P

BF, F32 = jnp.bfloat16, jnp.float32
TB = 512
CB = 768
NN, NT, TN = ((1,), (0,)), ((1,), (1,)), ((0,), (0,))
MESH = pl.DeviceIdType.MESH
DMA = pltpu.SemaphoreType.DMA


def dot(a, b, dims=NN):
    return lax.dot_general(a, b, (dims, ((), ())), preferred_element_type=F32)


def normed(h):
    wide = h.astype(F32)
    return (wide * lax.rsqrt(jnp.mean(wide**2, -1, keepdims=True) + 1e-6)).astype(BF)


def chip_peers():
    chip = lax.axis_index("chip")
    return chip + 1 - 2 * lax.rem(chip, 2), lax.rem(chip + 2, 4), 3 - chip


def z_peers():
    z = lax.axis_index("r")
    return z + 1 - 2 * lax.rem(z, 2), lax.rem(z + 2, 4)


def to_z(peer, **kw):
    return pltpu.make_async_remote_copy(device_id={"r": peer}, device_id_type=MESH, **kw)


def to_chip(peer, **kw):
    return pltpu.make_async_remote_copy(device_id={"chip": peer}, device_id_type=MESH, **kw)


def to_partner(**kw):
    return pltpu.make_async_remote_copy(device_id={"core": 1 - lax.axis_index("core")}, device_id_type=MESH, **kw)


def enter():
    barrier = pltpu.get_barrier_semaphore()
    for peer in chip_peers():
        pl.semaphore_signal(barrier, inc=1, device_id={"chip": peer}, device_id_type=MESH)
    pl.semaphore_signal(barrier, inc=1, device_id={"core": 1 - lax.axis_index("core")}, device_id_type=MESH)
    for peer in z_peers():
        pl.semaphore_signal(barrier, inc=1, device_id={"r": peer}, device_id_type=MESH)
    pl.semaphore_wait(barrier, 6)


class Gather:
    def __init__(self, *parts):
        self.rows, self.parts = parts[0][0].shape[1], parts
        self.ins = [(w, (1, *w.shape[1:]), lambda *_, l=l: (l, 0, 0)) for w, l, *_ in parts]
        self.outs = [((8 * self.rows, sum(p[3] for p in parts)), BF, None, None)]
        n = len(parts)
        self.scratch = [DMA((3, n)), DMA((3, n)), DMA((4, n)), DMA((4, n)), DMA((n,))]

    def bind(self, ins, outs, scratch):
        (self.full,) = outs
        chip, core = lax.axis_index("chip"), lax.axis_index("core")
        send, recv, psend, precv, local = scratch
        self.out, self.on, self.own, at = [], [], [], 0
        for k, (shard, (_, _, column, width)) in enumerate(zip(ins, self.parts)):

            def place(chip, core, at=at, width=width):
                first = pl.multiple_of((chip * 2 + core) * self.rows, self.rows)
                return self.full.at[pl.ds(first, self.rows), pl.ds(at, width)]

            mine, here = shard.at[0, :, pl.ds(column, width)], place(chip, core)
            self.own.append(to_partner(src_ref=mine, dst_ref=here, send_sem=psend.at[3, k], recv_sem=precv.at[3, k]))
            self.own.append(pltpu.make_async_copy(mine, here, local.at[k]))
            for i, peer in enumerate(chip_peers()):
                there = place(peer, core)
                self.out.append(to_chip(peer, src_ref=mine, dst_ref=here, send_sem=send.at[i, k], recv_sem=recv.at[i, k]))
                self.on.append(to_partner(src_ref=there, dst_ref=there, send_sem=psend.at[i, k], recv_sem=precv.at[i, k]))
            at += width

    def before(self, step, steps):
        if step == 0:
            for copy in self.out + self.own:
                copy.start()

    def after(self, step, steps):
        if step == steps - 2:
            self.forward()
        if step == steps - 1:
            self.finish()

    def forward(self):
        for copy, on in zip(self.out, self.on):
            copy.wait_recv()
            on.start()

    def finish(self):
        for copy in self.out:
            copy.wait_send()
        for copy in self.on + self.own:
            copy.wait()


class Reduce:
    def __init__(self, source, *stages):
        self.stages, shape = stages, source.shape[-2:]
        self.ins = [(source, None, None)]
        self.outs = [(shape, BF, shape, lambda *_: (0, 0))]
        n = len(stages)
        self.scratch = [pltpu.VMEM((n, *shape), BF), DMA]
        for kind, _ in stages:
            k = 3 if kind == "chips" else 1
            self.scratch += [pltpu.VMEM((k, *shape), BF), DMA((k,)), DMA((k,))]

    def bind(self, ins, outs, scratch):
        (source,), (self.result,) = ins, outs
        self.own, local, *rest = scratch
        first = source.at[lax.axis_index("chip")] if self.stages[0][0] == "chips" else source
        self.load = pltpu.make_async_copy(first, self.own.at[0], local)
        self.copies, self.got = [], []
        for j, (kind, _) in enumerate(self.stages):
            got, send, recv = rest[3 * j : 3 * j + 3]
            self.got.append(got)
            if kind == "chips":
                self.copies.append(
                    [
                        to_chip(peer, src_ref=source.at[peer], dst_ref=got.at[i], send_sem=send.at[i], recv_sem=recv.at[i])
                        for i, peer in enumerate(chip_peers())
                    ]
                )
            else:
                here = source if j == 0 else self.own.at[j]
                self.copies.append([to_z(z_peers()[kind], src_ref=here, dst_ref=got.at[0], send_sem=send.at[0], recv_sem=recv.at[0])])

    def add(self, j):
        if j == 0:
            self.load.wait()
        for copy in self.copies[j]:
            copy.wait()
        total = self.own[j].astype(F32)
        for i in range(len(self.copies[j])):
            total += self.got[j][i].astype(F32)
        if j + 1 < len(self.stages):
            self.own[j + 1] = total.astype(BF)
        else:
            self.result[...] = total.astype(BF)

    def before(self, step, steps):
        if step == 0:
            self.load.start()
            for copy in self.copies[0]:
                copy.start()
        for j, (_, when) in enumerate(self.stages):
            if when == step:
                self.add(j)

    def after(self, step, steps):
        for j, (_, when) in enumerate(self.stages):
            if when == step:
                for copy in self.copies[j + 1]:
                    copy.start()
            if when is None and step == steps - 1:
                self.add(j)


def pair_sum(acc, sums_ref, sent, got, send, recv):
    core = lax.axis_index("core")
    chips, rows = sums_ref.shape[:2]

    def rows_of(chip, core):
        return acc[pl.ds(pl.multiple_of((chip * 2 + core) * rows, rows), rows), :]

    copies = [
        to_partner(src_ref=sent.at[chip], dst_ref=got.at[chip], send_sem=send.at[chip], recv_sem=recv.at[chip]) for chip in range(chips)
    ]
    for chip in range(chips):
        sent[chip] = rows_of(chip, 1 - core).astype(BF)
        copies[chip].start()
    for chip in range(chips):
        copies[chip].wait()
        sums_ref[chip] = (rows_of(chip, core) + got[chip].astype(F32)).astype(BF)


def pair_scratch(rows, n):
    return [pltpu.VMEM((4, rows, n), BF)] * 2 + [DMA((4,))] * 2


def call(kernel, grid, ins, outs, scratch, flops, number, moves=(), aliases=None, steered=False, name=None):
    def spec(block, index):
        return pl.BlockSpec(memory_space=pl.ANY) if block is None else pl.BlockSpec(block, index)

    n_in, n_out, n_scratch = len(ins), len(outs), len(scratch)
    all_ins = list(ins) + [a for m in moves for a in m.ins]
    all_outs = list(outs) + [a for m in moves for a in m.outs]
    all_scratch = list(scratch) + [a for m in moves for a in m.scratch]

    def body(*refs):
        ins_, outs_, scratch_ = refs[: len(all_ins)], refs[len(all_ins) : len(all_ins) + len(all_outs)], refs[len(all_ins) + len(all_outs) :]
        i, o, c = n_in, n_out, n_scratch
        for m in moves:
            m.bind(ins_[i : i + len(m.ins)], outs_[o : o + len(m.outs)], scratch_[c : c + len(m.scratch)])
            i, o, c = i + len(m.ins), o + len(m.outs), c + len(m.scratch)
        if number is not None:

            @pl.when(functools.reduce(lambda a, b: a & b, [pl.program_id(k) == 0 for k in range(len(grid))]))
            def _():
                enter()

        if steered or not moves:
            kernel(*ins_[:n_in], *outs_[:n_out], *scratch_[:n_scratch], *moves)
            return

        def at_steps(do):
            for step in steps:

                @pl.when(pl.program_id(0) == step)
                def _():
                    for m in moves:
                        getattr(m, do)(step, grid[0])

        steps = sorted({0, grid[0] - 2, grid[0] - 1} | {when for m in moves for _, when in getattr(m, "stages", ()) if when is not None})
        at_steps("before")
        kernel(*ins_[:n_in], *outs_[:n_out], *scratch_[:n_scratch])
        at_steps("after")

    size = sum(a.size * a.dtype.itemsize for a, *_ in ins)
    return pl.pallas_call(
        body,
        grid=grid,
        in_specs=[spec(b, i) for _, b, i in all_ins],
        out_specs=[spec(b, i) for *_, b, i in all_outs],
        out_shape=[jax.ShapeDtypeStruct(s, d) for s, d, *_ in all_outs],
        scratch_shapes=all_scratch,
        input_output_aliases=aliases or {},
        cost_estimate=pl.CostEstimate(flops=flops, bytes_accessed=size, transcendentals=0),
        compiler_params=pltpu.CompilerParams(
            vmem_limit_bytes=62 * 2**20,
            dimension_semantics=("arbitrary",) * len(grid),
            collective_id=number,
            has_side_effects=number is not None,
        ),
        name=name,
    )(*[a for a, *_ in all_ins])


def fwd_kernel(x_ref, gate_ref, up_ref, p_ref, a_ref, h_ref, a2_ref, w, wd, a_all, p_all, local, *moves):
    c, t = pl.program_id(0), pl.program_id(1)
    nt, nc = pl.num_programs(1), len(moves) - 3
    late = 2

    def fetch(full, to):
        copy = pltpu.make_async_copy(full, to, local)
        copy.start()
        copy.wait()

    for i, move in enumerate(moves):

        @pl.when((c == 0) & (t == 0))
        def _():
            move.before(0, 1)
            if i == 0:
                move.forward()

        if 0 < i <= nc:

            @pl.when((c == i - 1) & (t == nt - late))
            def _():
                move.forward()

        if i == nc + 1:

            @pl.when((c == nc) & (t == nt - late))
            def _():
                move.forward()

        if i <= nc:

            @pl.when((c == i) & (t == 0))
            def _():
                move.finish()
                fetch(move.full, w if i < nc else wd)

    rows = pl.ds(pl.multiple_of(t * TB, TB), TB)

    @pl.when(c == 0)
    def _():
        a = normed(x_ref[...])
        a_ref[...] = a
        a_all[rows, :] = a

    @pl.when(c < nc)
    def _():
        a = a_all[rows, :]
        gate, up = dot(a, w[:, :CB]), dot(a, w[:, CB:])
        gate_ref[...], up_ref[...] = gate, up
        p = (gate * jax.nn.sigmoid(gate) * up).astype(BF)
        p_ref[...] = p
        p_all[jnp.minimum(c, nc - 1), rows, :] = p

    @pl.when(c == nc)
    def _():
        h = x_ref[...] + sum(dot(p_all[i, rows, :], wd[i * CB : (i + 1) * CB, :]) for i in range(nc)).astype(BF)
        h_ref[...] = h
        a2_ref[...] = normed(h)

        @pl.when(t == nt - 1)
        def _():
            moves[-1].forward()
            for move in moves[nc + 1 :]:
                move.finish()


def back_kernel(saved, n_alias, *refs):
    refs = list(refs)
    a_ref, dh_ref, wd_ref = refs[:3]
    given = refs[3:5] if saved else refs[3:4]
    refs = refs[3 + len(given) + n_alias :]
    d_ref = refs.pop(0)
    p_ref = None if saved else refs.pop(0)
    sums_ref, acc, *pair = refs
    t = pl.program_id(0)

    @pl.when(t == 0)
    def _():
        acc[...] = jnp.zeros_like(acc)

    part = TB // 2 if saved else TB
    for i in range(0, TB, part):
        rows = slice(i, i + part)
        a = a_ref[rows, :]
        if saved:
            gate, up = given[0][rows, :], given[1][rows, :]
        else:
            gate, up = dot(a, given[0][:, :CB]), dot(a, given[0][:, CB:])
        dp = dot(dh_ref[rows, :], wd_ref[...], NT).astype(BF).astype(F32)
        sig = jax.nn.sigmoid(gate)
        silu = gate * sig
        d_ref[rows, :CB] = (dp * up * (sig + silu * (1 - sig))).astype(BF)
        d_ref[rows, CB:] = (dp * silu).astype(BF)
        if not saved:
            p_ref[rows, :] = (silu * up).astype(BF)
    acc[...] += dot(a_ref[...], d_ref[...], TN)

    @pl.when(t == pl.num_programs(0) - 1)
    def _():
        pair_sum(acc, sums_ref, *pair)


def down_back_kernel(p_ref, dh_ref, sums_ref, acc, *pair):
    t = pl.program_id(0)

    @pl.when(t == 0)
    def _():
        acc[...] = jnp.zeros_like(acc)

    acc[...] += dot(p_ref[...], dh_ref[...], TN)

    @pl.when(t == pl.num_programs(0) - 1)
    def _():
        pair_sum(acc, sums_ref, *pair)


def input_back_kernel(d_ref, h_ref, dh_ref, *refs):
    *weights, out_ref = refs
    da = sum(dot(d_ref[:, 2 * CB * c : 2 * CB * (c + 1)], w[...], NT) for c, w in enumerate(weights)).astype(BF)
    g, h = da.astype(F32), h_ref[...].astype(F32)
    scale = lax.rsqrt(jnp.mean(h**2, -1, keepdims=True) + 1e-6)
    dn = g * scale - h * (scale**3 * jnp.mean(g * h, -1, keepdims=True))
    out_ref[...] = dh_ref[...] + dn.astype(BF)


def stack_kernel(*refs):
    *chunks, d0, d1, dg, du, dd = refs
    nc = len(chunks) // 2
    for i, ref in enumerate(chunks):
        at = slice(i % nc * CB, (i % nc + 1) * CB)
        dg[i // nc, :, at] = ref[:, :CB]
        du[i // nc, :, at] = ref[:, CB:]
    dd[0], dd[1] = d0[...], d1[...]


def solution(mesh):
    sizes = mesh.shape
    rep, r, s = sizes["rep"], sizes["r"], sizes["s"]
    fine = Mesh(mesh.devices.reshape(rep, r, s // 2, 2), ("rep", "r", "chip", "core"))

    def step(x, dy, w_gate, w_up, w_down):
        x, dy = x[0], dy[0]
        tokens, d = x.shape
        layers, _, ff = w_gate.shape
        nt, nc = tokens // TB, ff // CB
        row = lambda t: (t, 0)
        rows_d, rows_f = d // s, ff // s
        mm = 2 * tokens * d * ff
        blockrow = (TB, d)
        state = ((tokens, d), BF, blockrow, row)
        numbers = iter(range(100))

        def chunk(l, c):
            return Gather((w_gate, l, c * CB, CB), (w_up, l, c * CB, CB))

        def down(l):
            return Gather((w_down, l, 0, d))

        first = lambda c, t: (jnp.where(c == 0, t, nt - 1), 0)
        ends = lambda c, t: (jnp.where((c == 0) | (c == nc), t, nt - 1), 0)
        then = lambda c, t: (jnp.where(c == nc, t, 0), 0)
        chunked = lambda c, t: (jnp.where(c < nc, t, nt - 1), jnp.minimum(c, nc - 1))
        gate, up, p1, a1, h1, a2, *full = call(
            fwd_kernel,
            (nc + 1, nt),
            [(x, blockrow, ends)],
            [((tokens, ff), dt, (TB, CB), chunked) for dt in (F32, F32, BF)] + [((tokens, d), BF, blockrow, i) for i in (first, then, then)],
            [pltpu.VMEM((d, 2 * CB), BF), pltpu.VMEM((ff, d), BF), pltpu.VMEM((tokens, d), BF), pltpu.VMEM((nc, tokens, CB), BF), DMA],
            3 * mm,
            next(numbers),
            [chunk(0, c) for c in range(nc)] + [down(0), down(1), chunk(1, 0)],
            steered=True,
            name="fwd",
        )
        gu1, (wd1, wd2, gu2_0) = full[:nc], full[nc:]

        def back(c, a, dh, wd, so_far, moves, w=None):
            here = lambda t: (t, c)
            ins = [(a, blockrow, row), (dh, blockrow, row), (wd, (CB, d), lambda t: (c, 0))]
            outs = [((tokens, 2 * ff), BF, (TB, 2 * CB), here)]
            if w is None:
                ins += [(gate, (TB, CB), here), (up, (TB, CB), here)]
            else:
                ins += [(w, (d, 2 * CB), lambda t: (0, 0))]
                outs += [((tokens, ff), BF, (TB, CB), here)]
            aliases = {len(ins) + i: i for i in range(len(so_far))}
            ins += [(buffer, None, None) for buffer in so_far]
            n = len(outs)
            outs += [((4, rows_d, 2 * CB), BF, (4, rows_d, 2 * CB), lambda t: (0, 0, 0))]
            got = call(
                functools.partial(back_kernel, w is None, len(so_far)),
                (nt,),
                ins,
                outs,
                [pltpu.VMEM((d, 2 * CB), F32)] + pair_scratch(rows_d, 2 * CB),
                (3 if w is None else 5) * mm // nc,
                next(numbers),
                moves,
                aliases,
                name="back",
            )
            return got[:n], got[n], got[n + 1 :]

        def down_back(p, dh, moves):
            return call(
                down_back_kernel,
                (nt,),
                [(p, (TB, ff), row), (dh, blockrow, row)],
                [((4, rows_f, d), BF, (4, rows_f, d), lambda t: (0, 0, 0))],
                [pltpu.VMEM((ff, d), F32)] + pair_scratch(rows_f, d),
                mm,
                next(numbers),
                moves,
                name="down_back",
            )

        def input_back(dgu, h, dh, ws, moves=()):
            return call(
                input_back_kernel,
                (nt,),
                [(dgu, (TB, 2 * ff), row), (h, blockrow, row), (dh, blockrow, row)] + [(w, w.shape, lambda t: (0, 0)) for w in ws],
                [state],
                [],
                2 * mm,
                next(numbers) if moves else None,
                moves,
                name="input_back",
            )

        so_far, s20, (gu2_1, gu2_2) = back(0, a2, dy, wd2, [], [chunk(1, 1), chunk(1, 2)], gu2_0)
        so_far, s21, (u20,) = back(1, a2, dy, wd2, so_far, [Reduce(s20, ("chips", None))], gu2_1)
        (dgu2, p2), s22, (t20, u21) = back(
            2, a2, dy, wd2, so_far, [Reduce(u20, (0, 3), (1, None)), Reduce(s21, ("chips", None))], gu2_2
        )
        s2d, t21, u22 = down_back(p2, dy, [Reduce(u21, (0, 3), (1, None)), Reduce(s22, ("chips", None))])
        dh1, t22, u2d = input_back(dgu2, h1, dy, [gu2_0, gu2_1, gu2_2], [Reduce(u22, (0, 3), (1, None)), Reduce(s2d, ("chips", None))])
        s1d, v2d = down_back(p1, dh1, [Reduce(u2d, (0, None))])
        so_far, s10, (t2d, u1d) = back(0, a1, dh1, wd1, [], [Reduce(v2d, (1, None)), Reduce(s1d, ("chips", None))])
        so_far, s11, (t1d, u10) = back(1, a1, dh1, wd1, so_far, [Reduce(u1d, (0, 2), (1, None)), Reduce(s10, ("chips", None))])
        (dgu1,), s12, (t10, u11) = back(2, a1, dh1, wd1, so_far, [Reduce(u10, (0, 2), (1, None)), Reduce(s11, ("chips", None))])
        dx, t11, t12 = input_back(dgu1, x, dh1, gu1, [Reduce(u11, (0, 2), (1, None)), Reduce(s12, ("chips", 3), (0, 5), (1, None))])

        w_out = [((layers, rows_d, ff), BF)] * 2 + [((layers, rows_f, d), BF)]
        terms = (t10, t11, t12, t20, t21, t22, t1d, t2d)
        dg, du, dd = call(
            stack_kernel,
            (1,),
            [(t, t.shape, lambda _: (0, 0)) for t in terms],
            [(shape, dt, shape, lambda _: (0, 0, 0)) for shape, dt in w_out],
            [],
            10**6,
            None,
            name="stack",
        )
        return dx[None], dg, du, dd

    states, cut = P(("rep", "r", "chip", "core"), None, None), P(None, ("chip", "core"), None)
    return jax.shard_map(
        step,
        mesh=fine,
        in_specs=(states, states) + (cut,) * 3,
        out_specs=(states,) + (P("rep", ("chip", "core"), None),) * 3,
        check_vma=False,
    )
```
